256 devices in a mesh: section: 8 (over z_hi, core), row: 4 (over x), col: 8 (over y, z_lo).
Axes of the slice: x: 4, y: 4, z: 8 (z_hi: 4, z_lo: 2; z = z_hi * 2 + z_lo), core: 2. Of those that a mesh axis runs over, the one named last changes fastest.
Arguments:
- coeffs: bfloat16 [8, 4096, 6144], P('section', 'row', 'col'), may hold values from -0.109375 to 0.109375
- occ_energy: float32 [8], P('section'), may hold values from -1 to -0.3
- vir_energy: float32 [4096], P('row'), may hold values from 0.1 to 4
- frequency: float32 [], replicated, may hold values from 0.3 to 3
Outputs:
- response: float32 [6144, 6144], P(('section', 'row'), 'col')
The draws below stay inside these ranges and needn't reach their ends.
All inputs are finite; a program needn't handle non-finite values.
Results may differ from the reference program's by a relative error of at most 0.0012.
Values may be sent and summed in bfloat16 or wider, within the bound.
No kernel may reach another device: no remote copies, remote signals or barrier semaphores. Data moves between devices by JAX's collectives and lax.ppermute only.
A program may use at most 128 MiB of HBM per device.

```python
import math
import jax
import jax.numpy as jnp
from jax import lax

NAUX = 6144
NVIR = 4096
NOCC = 8


def strengthened(array, own_key, source, target, parts, factor):
    def block_of(axis_at):
        return (jnp.arange(array.shape[axis_at]) // (array.shape[axis_at] // parts)).reshape((-1,) + (1,) * (array.ndim - 1 - axis_at))

    near = jax.random.permutation(own_key, parts)[block_of(target)]
    second = (block_of(target) + parts // 2) % parts
    return jnp.where((block_of(source) == near) | (block_of(source) == second), factor * array, array)


def levels(stream_key, extent, split, low, high):
    gain, own = 1.0, jax.random.fold_in(stream_key, 6)
    for dim, blocks in split:
        draws = jnp.exp(jax.random.uniform(jax.random.fold_in(own, dim), (blocks,), jnp.float32, low / len(split), high / len(split)))
        gain = gain * jnp.repeat(draws, extent[dim] // blocks).reshape([-1 if axis == dim else 1 for axis in range(len(extent))])
    return gain


def bell_draw_with(rng, dims, deviation, reach, shards, heavy, kind=jnp.bfloat16):
    array = deviation * jax.random.normal(rng, dims, jnp.float32)
    if shards:
        array = array * levels(rng, dims, shards, -0.22, 0.18)
    return jnp.clip(strengthened(array, jax.random.fold_in(rng, 3), *heavy), -reach, reach).astype(kind)


def setup_inputs(seed: int = 0) -> dict:
    seeds = jax.random.split(jax.random.key(seed), 5)
    return {
        "coeffs": bell_draw_with(seeds[0], (NOCC, NVIR, NAUX), ((NOCC * NVIR) ** -0.5), 0.109375, ((0, 8), (1, 4), (2, 8)), (0, 2, 8, 2.0)),
        "occ_energy": jnp.clip(-1.0 + 0.7 * jax.random.uniform(seeds[1], (NOCC,), jnp.float32) ** levels(seeds[1], (NOCC,), ((0, 8),), -0.2, 0.2), -1.0, -0.3),
        "vir_energy": jnp.clip(jnp.exp(math.log(4.0) - 3.6888794 * jax.random.uniform(seeds[2], (NVIR,), jnp.float32) ** levels(seeds[2], (NVIR,), ((0, 4),), -0.2, 0.2)), 0.1, 4.0),
        "frequency": jnp.clip(jnp.exp(jax.random.uniform(seeds[3], (), jnp.float32, math.log(0.3), math.log(3.0))), 0.3, 3.0),
    }


def reference(coeffs, occ_energy, vir_energy, frequency):
    def add_orbital(running, inputs):
        orbital_rows, energy = inputs
        energy_gap = vir_energy - energy
        factor = 2.0 * energy_gap / (energy_gap * energy_gap + frequency * frequency)
        scaled = (orbital_rows.astype(jnp.float32) * factor[:, None]).astype(jnp.bfloat16)
        running = running + jnp.dot(scaled.astype(jnp.float32).T, orbital_rows.astype(jnp.float32), precision=lax.Precision.HIGHEST)
        return running, None

    start_sum = jnp.zeros((NAUX, NAUX), jnp.float32)
    running, unused = lax.scan(add_orbital, start_sum, (coeffs, occ_energy))
    return running
```

```python
import jax
import jax.numpy as jnp
from jax import lax
from jax.sharding import Mesh
from jax.sharding import PartitionSpec as P


COL = ("y", "z_lo")
SECTION = ("z_hi", "core")


def shift_of(count, step):
    return [(source, (source + step) % count) for source in range(count)]


def pair_sum(left, right):
    return jnp.einsum("sap,saq->pq", left, right, preferred_element_type=jnp.float32)


def per_device(coeffs, occ_energy, vir_energy, frequency):
    z_hi, core, row, y, z_lo = (lax.axis_index(name) for name in ("z_hi", "core", "row", "y", "z_lo"))
    rows = lax.axis_size("row")
    sides = lax.axis_size("y")
    own = coeffs[0]
    virs, width = own.shape
    part = width // rows

    upper = (y >= sides // 2).astype(jnp.int32)
    half_sent = lax.dynamic_slice_in_dim(own, (1 - upper) * (virs // 2), virs // 2, 0)
    occ_other = lax.ppermute(occ_energy, "core", shift_of(2, 1))
    own_other = lax.ppermute(own, "core", shift_of(2, 1))
    beside = lax.ppermute(own, "z_lo", shift_of(2, 1))
    next_one = lax.ppermute(own, "y", shift_of(sides, -1))
    next_two = lax.ppermute(lax.ppermute(half_sent, "y", shift_of(sides, 1)), "y", shift_of(sides, 1))
    beside_other = lax.ppermute(beside, "core", shift_of(2, 1))
    one_other = lax.ppermute(next_one, "core", shift_of(2, 1))
    two_other = lax.ppermute(next_two, "core", shift_of(2, 1))

    occupied = jnp.concatenate([occ_energy, occ_other])
    energy_gap = vir_energy[None, :] - occupied[:, None]
    factor = 2.0 * energy_gap / (energy_gap * energy_gap + frequency * frequency)

    right_own = jnp.stack([own, own_other])
    left = jnp.where(core == z_lo, right_own, jnp.stack([beside, beside_other]))
    left = (left.astype(jnp.float32) * factor[:, :, None]).astype(jnp.bfloat16)
    left_half = lax.dynamic_slice_in_dim(left, upper * (virs // 2), virs // 2, 1)
    tiles = [
        pair_sum(left, right_own),
        pair_sum(left, jnp.stack([next_one, one_other])),
        pair_sum(left_half, jnp.stack([next_two, two_other])),
    ]

    summed = []
    for tile in tiles:
        tile = tile.reshape(rows, part, width)
        total = lax.dynamic_index_in_dim(tile, row, 0, keepdims=False)
        for step in range(1, rows):
            sent = lax.dynamic_index_in_dim(tile, (row + step) % rows, 0, keepdims=False).astype(jnp.bfloat16)
            total = total + lax.ppermute(sent, "row", shift_of(rows, step)).astype(jnp.float32)
        summed.append(total)

    stacked = jnp.stack(summed)
    ahead = (z_hi - y) % sides
    held = lax.dynamic_index_in_dim(stacked, jnp.minimum(ahead, 2), 0, keepdims=False)
    held = jnp.where(ahead < 3, held, 0.0)
    for step in range(1, sides):
        which = (z_hi + step - y) % sides
        sent = lax.dynamic_index_in_dim(stacked, jnp.minimum(which, 2), 0, keepdims=False)
        pairs = [
            (a * sides + b, ((a + step) % sides) * sides + b)
            for a in range(sides) for b in range(sides) if (a + step - b) % sides != 3
        ]
        held = held + lax.ppermute(sent, ("z_hi", "y"), pairs)

    swaps = [
        (b * sides + a, a * sides + b)
        for a in range(sides) for b in range(sides) if (a - b) % sides in (2, 3)
    ]
    swapped = lax.ppermute(held, ("z_hi", "y"), swaps)
    blocks = held.reshape(part, rows, part).transpose(1, 0, 2)
    turned = jnp.zeros_like(blocks)
    names = ("z_hi", "core", "row", "y", "z_lo")
    for step in range(rows):
        pairs = []
        for a in range(sides):
            for b in range(sides):
                if (a - b) % sides not in (1, 2):
                    continue
                for k in range(2):
                    for l in range(2):
                        for r in range(rows):
                            index = lambda k, r, l: (((a * 2 + k) * rows + r) * sides + b) * 2 + l
                            pairs.append((index(k, r, l), index(l, (r + step) % rows, k)))
        sent = lax.dynamic_index_in_dim(blocks, (row + step) % rows, 0, keepdims=False)
        got = lax.ppermute(sent, names, pairs)
        turned = lax.dynamic_update_index_in_dim(turned, got, (row - step) % rows, 0)
    turned = turned.transpose(2, 0, 1).reshape(part, width)
    mirrored = jnp.where(ahead == 1, turned, jnp.where(ahead == 2, swapped + turned, swapped))
    return jnp.where(ahead == 0, held, mirrored)


def solution(mesh):
    torus = Mesh(
        mesh.devices.reshape(mesh.shape["section"] // 2, 2, mesh.shape["row"], mesh.shape["col"] // 2, 2),
        ("z_hi", "core", "row", "y", "z_lo"),
    )
    in_specs = (P(SECTION, "row", COL), P(SECTION), P("row"), P())
    out_specs = P(SECTION + ("row",), COL)
    return jax.shard_map(
        per_device, mesh=torus, in_specs=in_specs, out_specs=out_specs, check_vma=False
    )
```
